32 devices in a mesh: tm: 16 (over z, y, core), chan: 2 (over x).
Axes of the slice: x: 2, y: 2, z: 4, core: 2. Of those that a mesh axis runs over, the one named last changes fastest.
Arguments:
- signal: bfloat16 [32768, 512], P('tm', 'chan'), may hold values from -72 to 72
- tapers: bfloat16 [8, 4096], replicated, may hold values from -0.09375 to 0.09375
- eigenvalues: float32 [8], replicated, may hold values from 0.05 to 1
Outputs:
- relative_psd: float32 [2048, 512], P('tm', 'chan')
The draws below stay inside these ranges and needn't reach their ends.
All inputs are finite; a program needn't handle non-finite values.
Results may differ from the reference program's by a relative error of at most 0.0026.
The reference program's roundings to bfloat16 on the way count: a program that leaves them out, or rounds other values in their place, can miss the bound.
Values may be sent and summed in bfloat16 or wider, within the bound.
No kernel may reach another device: no remote copies, remote signals or barrier semaphores. Data moves between devices by JAX's collectives and lax.ppermute only.
A program may use at most 64 MiB of HBM per device.

```python
import math
import jax
import jax.numpy as jnp
from jax import lax

P_SIZE = 32
Q = 128
TAPERS = 8
SEG = 4096
CHANNELS = 512
TIME = 32768


def draw_signal(key, part):
    noise_key = jax.random.fold_in(key, 11)
    offset_key = jax.random.fold_in(key, 23)
    time_pos = jnp.arange(TIME, dtype=jnp.float32)[:, None]
    chan_pos = jnp.arange(CHANNELS, dtype=jnp.float32)[None, :]
    growth = (1.0 + 2.0 * time_pos / TIME) * (1.0 + 2.0 * chan_pos / CHANNELS)
    offset = jax.random.uniform(offset_key, (1, CHANNELS), jnp.float32, -2.0, 2.0)
    noise = jnp.clip(jax.random.normal(noise_key, (TIME, CHANNELS), jnp.float32), -6.0, 6.0)
    values = noise * growth + offset
    return values.astype(jnp.bfloat16)


def scatter_about(key, extent, scale, reach, kind=jnp.bfloat16):
    return jnp.clip(scale * jax.random.normal(key, extent, jnp.float32), -reach, reach).astype(kind)


def setup_inputs(seed: int = 0) -> dict:
    splits = jax.random.split(jax.random.key(seed), 4)
    signal = draw_signal(jax.random.fold_in(splits[3], 71), 0)
    tapers = scatter_about(splits[1], (TAPERS, SEG), SEG ** -0.5, 0.09375)
    eigenvalues = jnp.clip(jnp.exp(jax.random.uniform(splits[2], (TAPERS,), jnp.float32, math.log(0.05), math.log(1.0))), 0.05, 1.0)
    return dict(signal=signal, tapers=tapers, eigenvalues=eigenvalues)


EPSILON = 1e-6


def dft_tables():
    inner = jnp.arange(Q, dtype=jnp.int32)
    outer = jnp.arange(P_SIZE, dtype=jnp.int32)
    halves = jnp.arange(P_SIZE // 2, dtype=jnp.int32)
    angle_first = ((inner[:, None] * inner[None, :]) % Q).astype(jnp.float32) * (2.0 * math.pi / Q)
    first_table = jnp.concatenate([jnp.cos(angle_first), -jnp.sin(angle_first)], axis=0).astype(jnp.bfloat16)
    angle_twist = ((inner[:, None] * outer[None, :]) % (P_SIZE * Q)).astype(jnp.float32) * (2.0 * math.pi / (P_SIZE * Q))
    twist_cos = jnp.cos(angle_twist)[:, :, None]
    twist_sin = jnp.sin(angle_twist)[:, :, None]
    angle_last = ((outer[:, None] * halves[None, :]) % P_SIZE).astype(jnp.float32) * (2.0 * math.pi / P_SIZE)
    last_cos = jnp.cos(angle_last).astype(jnp.bfloat16)
    last_sin = jnp.sin(angle_last).astype(jnp.bfloat16)
    return first_table, twist_cos, twist_sin, last_cos, last_sin


def taper_power(tapered, tables):
    first_table, twist_cos, twist_sin, last_cos, last_sin = tables
    width = tapered.shape[1]
    columns = tapered.reshape(Q, P_SIZE * width)
    first = jnp.dot(first_table, columns, preferred_element_type=jnp.float32)
    first_real = first[:Q].reshape(Q, P_SIZE, width)
    first_imaginary = first[Q:].reshape(Q, P_SIZE, width)
    twist_real = (first_real * twist_cos + first_imaginary * twist_sin).astype(jnp.bfloat16).astype(jnp.float32)
    twist_imaginary = (first_imaginary * twist_cos - first_real * twist_sin).astype(jnp.bfloat16).astype(jnp.float32)
    cos_wide = last_cos.astype(jnp.float32)
    sin_wide = last_sin.astype(jnp.float32)
    last_real = jnp.einsum('pa,kpc->akc', cos_wide, twist_real) + jnp.einsum('pa,kpc->akc', sin_wide, twist_imaginary)
    last_imaginary = jnp.einsum('pa,kpc->akc', cos_wide, twist_imaginary) - jnp.einsum('pa,kpc->akc', sin_wide, twist_real)
    power = last_real * last_real + last_imaginary * last_imaginary
    return power.reshape((P_SIZE // 2) * Q, width)


def reference(signal, tapers, eigenvalues):
    samples = signal.astype(jnp.float32)
    common = jnp.sum(samples, axis=1) / CHANNELS
    referenced = (samples - common[:, None]).astype(jnp.bfloat16)
    widened = referenced.astype(jnp.float32)
    centre = jnp.sum(widened, axis=0) / TIME
    variance = jnp.sum((widened - centre) ** 2, axis=0) / TIME
    weights = eigenvalues / jnp.sum(eigenvalues)
    stride = SEG // 2
    segments = TIME // stride - 1
    tables = dft_tables()

    def accumulate(carry, seg_index):
        start = (seg_index * stride).astype(jnp.int32)
        window = lax.dynamic_slice_in_dim(referenced, start, SEG, 0).astype(jnp.float32) - centre
        for taper in range(TAPERS):
            tapered = (window * tapers[taper][:, None].astype(jnp.float32)).astype(jnp.bfloat16)
            carry = carry + weights[taper] * taper_power(tapered, tables)
        return carry, None

    initial = jnp.zeros((SEG // 2, CHANNELS), jnp.float32)
    total, _ = lax.scan(accumulate, initial, jnp.arange(segments, dtype=jnp.int32))
    return total / segments / (variance + EPSILON)
```

```python
import math

import jax
import jax.numpy as jnp
import numpy as np
from jax import lax
from jax.experimental import pallas as pl
from jax.experimental.pallas import tpu as pltpu
from jax.sharding import PartitionSpec as P

EPSILON = 1e-06
LANES = 128
R = 32
UNITS = R // 2
f32 = jnp.float32
bf16 = jnp.bfloat16

CONJ = {3: 29, 7: 25, 11: 21, 15: 17, 6: 26, 14: 18}


def unit_tables(seg, groups):
    half_m = seg // 2 // R
    per = half_m // groups
    n1 = np.arange(LANES)[:, None]
    col = np.arange(LANES)
    d = col // (2 * per)
    s = (col // per) % 2
    q = col % per
    m = d * per + q
    out = np.zeros((UNITS, 2 * LANES, 2 * LANES), np.float64)
    for u in range(UNITS):
        if u == 0:
            k = R * m + s * (R // 2)
            ang = 2 * np.pi * ((n1 * k) % seg) / seg
            for part in range(2):
                pick = (s == part)[None, :]
                rows = slice(part * LANES, (part + 1) * LANES)
                out[u, rows, :LANES] = np.cos(ang) * pick
                out[u, rows, LANES:] = -np.sin(ang) * pick
        else:
            k = np.where(s == 0, R * m + u, seg - (R * m + R - u))
            ang = 2 * np.pi * ((n1 * k) % seg) / seg
            sign = -1.0 if u in CONJ else 1.0
            out[u, :LANES, :LANES] = np.cos(ang)
            out[u, :LANES, LANES:] = -np.sin(ang)
            out[u, LANES:, :LANES] = sign * np.sin(ang)
            out[u, LANES:, LANES:] = sign * np.cos(ang)
    return out.astype(np.float32).astype(jnp.bfloat16)


def bin_rows(groups, seg):
    per = seg // 2 // R // groups
    rows = []
    for q in range(per):
        for b in range(R):
            if b < UNITS:
                u, s = b, 0
            elif b == UNITS:
                u, s = 0, 1
            else:
                u, s = R - b, 1
            rows.append(u * 2 * per + s * per + q)
    return rows


def cmul(a, angle):
    re, im = a
    c, s = math.cos(angle), math.sin(angle)
    return (re * c + im * s, im * c - re * s)


def rot45(a):
    h = math.sqrt(0.5)
    re, im = a
    return ((re + im) * h, (im - re) * h)


def rot135(a):
    h = math.sqrt(0.5)
    re, im = a
    return ((im - re) * h, (re + im) * -h)


def cadd(a, b):
    return (a[0] + b[0], a[1] + b[1])


def csub(a, b):
    return (a[0] - b[0], a[1] - b[1])


def fft4(c):
    e0, e1 = cadd(c[0], c[2]), csub(c[0], c[2])
    o0, o1 = cadd(c[1], c[3]), csub(c[1], c[3])
    return [
        cadd(e0, o0),
        (e1[0] + o1[1], e1[1] - o1[0]),
        csub(e0, o0),
        (e1[0] - o1[1], e1[1] + o1[0]),
    ]


def real_fft32(x, put):
    s0, s1, s2 = [], [], []
    for a in range(8):
        p, m = x[a] + x[a + 16], x[a] - x[a + 16]
        pb, mb = x[a + 8] + x[a + 24], x[a + 8] - x[a + 24]
        s0.append(p + pb)
        s2.append(p - pb)
        s1.append((m, mb))
    h = math.sqrt(0.5)
    t = [s0[n] + s0[n + 4] for n in range(4)]
    v = [s0[n] - s0[n + 4] for n in range(4)]
    e, o = t[0] + t[2], t[1] + t[3]
    put(0, e + o, e - o)
    put(8, t[0] - t[2], t[3] - t[1])
    a1, a3 = (v[1] - v[3]) * h, (v[1] + v[3]) * h
    put(4, v[0] + a1, -v[2] - a3)
    put(12, v[0] - a1, v[2] - a3)
    w = -2 * math.pi / 16
    c = [(s2[0], -s2[4])]
    for n in range(1, 4):
        c.append((s2[n], s2[n + 4]))

    def rotated(n):
        a, b = c[n]
        cs, sn = math.cos(2 * math.pi * n / 16), math.sin(2 * math.pi * n / 16)
        if n == 2:
            return ((a - b) * h, (a + b) * -h)
        return (a * cs - b * sn, a * -sn - b * cs)

    f = fft4([c[0], rotated(1), rotated(2), rotated(3)])
    put(2, *f[0])
    put(10, *f[1])
    put(14, *f[2])
    put(6, *f[3])
    g = [(s1[0][0], -s1[0][1])]
    for n in range(1, 8):
        a, b = s1[n]
        if n == 4:
            g.append(((a - b) * h, (a + b) * -h))
        else:
            cs, sn = math.cos(2 * math.pi * n / 32), math.sin(2 * math.pi * n / 32)
            g.append((a * cs - b * sn, a * -sn - b * cs))
    even = fft4([g[0], g[2], g[4], g[6]])
    odd = fft4([g[1], g[3], g[5], g[7]])
    o0 = odd[0]
    o1 = rot45(odd[1])
    o3 = rot135(odd[3])
    o2 = odd[2]
    put(1, *cadd(even[0], o0))
    put(15, *csub(even[0], o0))
    put(5, *cadd(even[1], o1))
    put(11, *csub(even[1], o1))
    put(9, even[2][0] + o2[1], even[2][1] - o2[0])
    put(7, even[2][0] - o2[1], even[2][1] + o2[0])
    put(13, *cadd(even[3], o3))
    put(3, *csub(even[3], o3))


def prep_kernel(own_ref, near_ref, common_ref, ref_ref, stats_ref):
    blocks = own_ref.shape[0] // LANES
    count = 2 * blocks * LANES

    def block(b, total):
        for h, src in enumerate((own_ref, near_ref)):
            x = src[pl.ds(pl.multiple_of(b * LANES, LANES), LANES), :].astype(f32).T
            x = (x - common_ref[h, pl.ds(b, 1), :]).astype(bf16)
            ref_ref[h, b] = x
            total = total + x.astype(f32)
        return total

    total = lax.fori_loop(0, blocks, block, jnp.zeros((LANES, LANES), f32))
    mean = jnp.sum(total, axis=1, keepdims=True) / count
    mean_wide = jnp.broadcast_to(mean, (LANES, LANES))

    def spread(b, acc):
        for h in range(2):
            d = ref_ref[h, b].astype(f32) - mean_wide
            acc = acc + d * d
        return acc

    acc = lax.fori_loop(0, blocks, spread, jnp.zeros((LANES, LANES), f32))
    stats_ref[0:1, :] = mean_wide.T[0:1, :]
    stats_ref[1:2, :] = jnp.sum(acc.T, axis=0, keepdims=True)


def main_kernel(order_ref, ref_ref, far_ref, far_common_ref, centre_ref, scale_ref, taps_ref,
                w_ref, out_ref, y_ref, ga_ref, gb_ref, acc_ref):
    blocks = ref_ref.shape[1]
    tapers = taps_ref.shape[1]
    groups = out_ref.shape[0]
    rows_per = LANES // groups
    chunks = 2 * LANES // 16
    centre = jnp.broadcast_to(centre_ref[...], (LANES, LANES)).T

    own_at = blocks
    near_at = order_ref[0] * blocks
    far_at = order_ref[1] * blocks

    def prepare(b, _):
        y_ref[own_at + b] = ref_ref[0, b].astype(f32) - centre
        y_ref[near_at + b] = ref_ref[1, b].astype(f32) - centre
        x = far_ref[pl.ds(pl.multiple_of(b * LANES, LANES), LANES), :].astype(f32).T
        x = (x - far_common_ref[pl.ds(b, 1), :]).astype(bf16).astype(f32)
        y_ref[far_at + b] = x - centre
        return 0

    lax.fori_loop(0, blocks, prepare, 0)
    acc_ref[...] = jnp.zeros(acc_ref.shape, f32)

    def first(r, taper, dst):
        seg = r // (chunks // 2)
        at = pl.multiple_of((r % (chunks // 2)) * 16, 16)
        row = pl.multiple_of(r * 16, 16)
        x = [
            y_ref[blocks * seg + n, pl.ds(at, 16), :] * taps_ref[seg, taper, n : n + 1, :]
            for n in range(R)
        ]

        def put(u, re, im):
            dst[u, pl.ds(row, 16), :LANES] = re.astype(bf16)
            dst[u, pl.ds(row, 16), LANES:] = im.astype(bf16)

        real_fft32(x, put)

    def second(u, src):
        z = jnp.dot(src[u], w_ref[u], preferred_element_type=f32)
        p = z * z
        p = p[:, :LANES] + p[:, LANES:]
        acc_ref[u] += p[:LANES] + p[LANES:]

    def both(taper, src, dst):
        def body(i, _):
            second(i, src)
            first(i, taper + 1, dst)
            return 0

        lax.fori_loop(0, UNITS, body, 0)

    def start(i, _):
        first(i, 0, ga_ref)
        return 0

    lax.fori_loop(0, chunks, start, 0)

    def pair(i, _):
        both(2 * i, ga_ref, gb_ref)
        both(2 * i + 1, gb_ref, ga_ref)
        return 0

    lax.fori_loop(0, tapers // 2 - 1, pair, 0)
    both(tapers - 2, ga_ref, gb_ref)

    def last(u, _):
        second(u, gb_ref)
        return 0

    lax.fori_loop(0, UNITS, last, 0)

    for u in range(UNITS):
        t = (acc_ref[u].T * scale_ref[...]).astype(bf16)
        for d in range(groups):
            out_ref[d, u * rows_per : (u + 1) * rows_per, :] = t[d * rows_per : (d + 1) * rows_per]


def merge_kernel(rows, parts_ref, out_ref, sum_ref):
    groups = parts_ref.shape[0]
    for parity in range(2):
        total = parts_ref[parity].astype(f32)
        for g in range(parity + 2, groups, 2):
            total = total + parts_ref[g].astype(f32)
        sum_ref[:, parity * LANES : (parity + 1) * LANES] = total
    for i, r in enumerate(rows):
        out_ref[i : i + 1, :] = sum_ref[r : r + 1, :]


def local(signal, tapers, eigenvalues):
    row_count, chan_count = signal.shape
    taper_count, seg = tapers.shape
    stride = seg // 2
    tm = lax.axis_size("tm")
    chans = lax.axis_size("chan")
    blocks = row_count // LANES
    all_rows = row_count * tm
    segments = all_rows // stride - 1
    half = chan_count // 2
    assert row_count == stride and half == LANES and seg == R * LANES
    index = lax.axis_index("tm")
    parity = index % 2

    near = [(i, i ^ 1) for i in range(tm)]
    far = [(i, i + 1 if i % 2 else i - 1) for i in range(1, tm - 1)]

    keep = lax.dynamic_slice_in_dim(signal, parity * half, half, 1)
    send = lax.dynamic_slice_in_dim(signal, (1 - parity) * half, half, 1)
    near_raw = lax.ppermute(send, "tm", near)
    far_raw = lax.ppermute(send, "tm", far)

    sums = jnp.sum(signal.astype(f32), axis=1).reshape(blocks, LANES)
    if chans == 2:
        total = sums + lax.ppermute(sums, "chan", [(0, 1), (1, 0)])
    else:
        total = lax.psum(sums, "chan")
    common = total / (chan_count * chans)
    common_near = lax.ppermute(common, "tm", near)
    common_far = lax.ppermute(common, "tm", far)

    referenced, stats = pl.pallas_call(
        prep_kernel,
        out_shape=(
            jax.ShapeDtypeStruct((2, blocks, LANES, LANES), bf16),
            jax.ShapeDtypeStruct((2, LANES), f32),
        ),
        name="prep",
    )(keep, near_raw, jnp.stack([common, common_near]))

    mean, spread = stats[0], stats[1]
    count = 2 * row_count
    step = 2
    while step < tm:
        other = lax.ppermute(jnp.stack([mean, spread]), "tm", [(i, i ^ step) for i in range(tm)])
        gap = other[0] - mean
        mean = (mean + other[0]) * 0.5
        spread = spread + other[1] + gap * gap * (count * 0.5)
        count *= 2
        step *= 2
    variance = spread / all_rows
    scale = 1.0 / (segments * (variance + EPSILON))

    weights = eigenvalues / jnp.sum(eigenvalues)
    valid = jnp.stack([index > 0, index < tm - 1]).astype(f32)
    taps = tapers.astype(f32) * jnp.sqrt(weights)[:, None]
    taps = (valid[:, None, None] * taps[None]).reshape(2, taper_count, R, LANES)
    order = jnp.stack([2 * (1 - parity), 2 * parity]).astype(jnp.int32)
    table = jnp.asarray(unit_tables(seg, tm))

    vmem = pl.BlockSpec(memory_space=pltpu.VMEM)
    parts = pl.pallas_call(
        main_kernel,
        out_shape=jax.ShapeDtypeStruct((tm, stride // tm, LANES), bf16),
        in_specs=[pl.BlockSpec(memory_space=pltpu.SMEM)] + [vmem] * 7,
        out_specs=vmem,
        scratch_shapes=[
            pltpu.VMEM((3 * blocks, LANES, LANES), f32),
            pltpu.VMEM((UNITS, 2 * LANES, 2 * LANES), bf16),
            pltpu.VMEM((UNITS, 2 * LANES, 2 * LANES), bf16),
            pltpu.VMEM((UNITS, LANES, LANES), f32),
        ],
        name="spectra",
    )(order, referenced, far_raw, common_far, mean[None], scale[None], taps, table)

    got = lax.all_to_all(parts, "tm", 0, 0, tiled=True)
    rows = bin_rows(tm, seg)
    return pl.pallas_call(
        lambda *refs: merge_kernel(rows, *refs),
        out_shape=jax.ShapeDtypeStruct((stride // tm, chan_count), f32),
        scratch_shapes=[pltpu.VMEM((stride // tm, chan_count), f32)],
        name="merge",
    )(got)


def solution(mesh):
    return jax.shard_map(
        local,
        mesh=mesh,
        in_specs=(P("tm", "chan"), P(), P()),
        out_specs=P("tm", "chan"),
        check_vma=False,
    )
```

```python
import functools
import math

import jax
import jax.numpy as jnp
import numpy as np
from jax import lax
from jax.experimental import pallas as pl
from jax.experimental.pallas import tpu as pltpu
from jax.sharding import PartitionSpec as P

EPSILON = 1e-06
LANES = 128
R = 32
UNITS = R // 2
UNROLL = 8
f32 = jnp.float32
bf16 = jnp.bfloat16

CONJ = {3: 29, 7: 25, 11: 21, 15: 17, 6: 26, 14: 18}


def unit_tables(seg, groups):
    half_m = seg // 2 // R
    per = half_m // groups
    n1 = np.arange(LANES)[:, None]
    col = np.arange(LANES)
    d = col // (2 * per)
    s = (col // per) % 2
    q = col % per
    m = d * per + q
    out = np.zeros((UNITS, 2 * LANES, 2 * LANES), np.float64)
    for u in range(UNITS):
        if u == 0:
            k = R * m + s * (R // 2)
            ang = 2 * np.pi * ((n1 * k) % seg) / seg
            for part in range(2):
                pick = (s == part)[None, :]
                rows = slice(part * LANES, (part + 1) * LANES)
                out[u, rows, :LANES] = np.cos(ang) * pick
                out[u, rows, LANES:] = -np.sin(ang) * pick
        else:
            k = np.where(s == 0, R * m + u, seg - (R * m + R - u))
            ang = 2 * np.pi * ((n1 * k) % seg) / seg
            sign = -1.0 if u in CONJ else 1.0
            out[u, :LANES, :LANES] = np.cos(ang)
            out[u, :LANES, LANES:] = -np.sin(ang)
            out[u, LANES:, :LANES] = sign * np.sin(ang)
            out[u, LANES:, LANES:] = sign * np.cos(ang)
    return out.astype(np.float32).astype(jnp.bfloat16)


def bin_rows(groups, seg):
    per = seg // 2 // R // groups
    rows = []
    for q in range(per):
        for b in range(R):
            if b < UNITS:
                u, s = b, 0
            elif b == UNITS:
                u, s = 0, 1
            else:
                u, s = R - b, 1
            rows.append(u * 2 * per + s * per + q)
    return rows


def cmul(a, angle):
    re, im = a
    c, s = math.cos(angle), math.sin(angle)
    return (re * c + im * s, im * c - re * s)


def rot45(a):
    h = math.sqrt(0.5)
    re, im = a
    return ((re + im) * h, (im - re) * h)


def rot135(a):
    h = math.sqrt(0.5)
    re, im = a
    return ((im - re) * h, (re + im) * -h)


def cadd(a, b):
    return (a[0] + b[0], a[1] + b[1])


def csub(a, b):
    return (a[0] - b[0], a[1] - b[1])


def fft4(c):
    e0, e1 = cadd(c[0], c[2]), csub(c[0], c[2])
    o0, o1 = cadd(c[1], c[3]), csub(c[1], c[3])
    return [
        cadd(e0, o0),
        (e1[0] + o1[1], e1[1] - o1[0]),
        csub(e0, o0),
        (e1[0] - o1[1], e1[1] + o1[0]),
    ]


def real_fft32(x, put):
    s0, s1, s2 = [], [], []
    for a in range(8):
        p, m = x[a] + x[a + 16], x[a] - x[a + 16]
        pb, mb = x[a + 8] + x[a + 24], x[a + 8] - x[a + 24]
        s0.append(p + pb)
        s2.append(p - pb)
        s1.append((m, mb))
    h = math.sqrt(0.5)
    t = [s0[n] + s0[n + 4] for n in range(4)]
    v = [s0[n] - s0[n + 4] for n in range(4)]
    e, o = t[0] + t[2], t[1] + t[3]
    put(0, e + o, e - o)
    put(8, t[0] - t[2], t[3] - t[1])
    a1, a3 = (v[1] - v[3]) * h, (v[1] + v[3]) * h
    put(4, v[0] + a1, -v[2] - a3)
    put(12, v[0] - a1, v[2] - a3)
    w = -2 * math.pi / 16
    c = [(s2[0], -s2[4])]
    for n in range(1, 4):
        c.append((s2[n], s2[n + 4]))

    def rotated(n):
        a, b = c[n]
        cs, sn = math.cos(2 * math.pi * n / 16), math.sin(2 * math.pi * n / 16)
        if n == 2:
            return ((a - b) * h, (a + b) * -h)
        return (a * cs - b * sn, a * -sn - b * cs)

    f = fft4([c[0], rotated(1), rotated(2), rotated(3)])
    put(2, *f[0])
    put(10, *f[1])
    put(14, *f[2])
    put(6, *f[3])
    g = [(s1[0][0], -s1[0][1])]
    for n in range(1, 8):
        a, b = s1[n]
        if n == 4:
            g.append(((a - b) * h, (a + b) * -h))
        else:
            cs, sn = math.cos(2 * math.pi * n / 32), math.sin(2 * math.pi * n / 32)
            g.append((a * cs - b * sn, a * -sn - b * cs))
    even = fft4([g[0], g[2], g[4], g[6]])
    odd = fft4([g[1], g[3], g[5], g[7]])
    o0 = odd[0]
    o1 = rot45(odd[1])
    o3 = rot135(odd[3])
    o2 = odd[2]
    put(1, *cadd(even[0], o0))
    put(15, *csub(even[0], o0))
    put(5, *cadd(even[1], o1))
    put(11, *csub(even[1], o1))
    put(9, even[2][0] + o2[1], even[2][1] - o2[0])
    put(7, even[2][0] - o2[1], even[2][1] + o2[0])
    put(13, *cadd(even[3], o3))
    put(3, *csub(even[3], o3))


def prep_kernel(signal_ref, common_ref, keep_ref, send_ref, keep_stats_ref, send_stats_ref):
    parity = lax.axis_index("tm") % 2
    blocks = keep_ref.shape[0]
    count = blocks * LANES
    sides = ((parity, keep_ref, keep_stats_ref), (1 - parity, send_ref, send_stats_ref))
    for side, dst, stats in sides:
        lanes = pl.ds(pl.multiple_of(side * LANES, LANES), LANES)
        total = jnp.zeros((LANES, LANES), f32)
        for b in range(blocks):
            x = signal_ref[b * LANES : (b + 1) * LANES, lanes].astype(f32).T
            x = (x - common_ref[b : b + 1, :]).astype(bf16)
            dst[b] = x
            total = total + x.astype(f32)
        mean = jnp.sum(total, axis=1, keepdims=True) / count
        mean_wide = jnp.broadcast_to(mean, (LANES, LANES))

        def spread(b, acc):
            d = dst[b].astype(f32) - mean_wide
            return acc + d * d

        acc = lax.fori_loop(0, blocks, spread, jnp.zeros((LANES, LANES), f32))
        stats[0:1, :] = mean_wide.T[0:1, :]
        stats[1:2, :] = jnp.sum(acc.T, axis=0, keepdims=True)


def main_kernel(segments, count, keep_ref, near_ref, far_ref, *refs):
    stats_refs = refs[:-8]
    taps_in_ref, w_ref, out_ref, taps_ref, y_ref, ga_ref, gb_ref, acc_ref = refs[-8:]
    index = lax.axis_index("tm")
    parity = index % 2
    blocks = keep_ref.shape[0]
    tapers = taps_ref.shape[1]
    groups = out_ref.shape[0]
    rows_per = LANES // groups
    chunks = 2 * LANES // 16

    parts = len(stats_refs)
    mean = stats_refs[0][0:1, :]
    for ref in stats_refs[1:]:
        mean = mean + ref[0:1, :]
    mean = mean / parts
    spread = jnp.zeros((1, LANES), f32)
    for ref in stats_refs:
        gap = ref[0:1, :] - mean
        spread = spread + ref[1:2, :] + gap * gap * count
    scale = 1.0 / (segments * (spread / (count * parts) + EPSILON))
    centre = jnp.broadcast_to(mean, (LANES, LANES)).T

    near_at = 2 * (1 - parity) * blocks
    far_at = 2 * parity * blocks

    def prepare(i, _):
        for j in range(4):
            b = 4 * i + j
            y_ref[blocks + b] = keep_ref[b].astype(f32) - centre
            y_ref[near_at + b] = near_ref[b].astype(f32) - centre
            y_ref[far_at + b] = far_ref[b].astype(f32) - centre
        return 0

    lax.fori_loop(0, blocks // 4, prepare, 0)
    first_valid = (index > 0).astype(f32)
    last_valid = (index < segments).astype(f32)
    taps_ref[0] = taps_in_ref[...] * first_valid
    taps_ref[1] = taps_in_ref[...] * last_valid
    acc_ref[...] = jnp.zeros(acc_ref.shape, f32)

    def first(r, taper, dst):
        seg = r // (chunks // 2)
        at = pl.multiple_of((r % (chunks // 2)) * 16, 16)
        row = pl.multiple_of(r * 16, 16)
        x = [
            y_ref[blocks * seg + n, pl.ds(at, 16), :] * taps_ref[seg, taper, n : n + 1, :]
            for n in range(R)
        ]

        def put(u, re, im):
            dst[u, pl.ds(row, 16), :LANES] = re.astype(bf16)
            dst[u, pl.ds(row, 16), LANES:] = im.astype(bf16)

        real_fft32(x, put)

    def second(u, src):
        z = jnp.dot(src[u], w_ref[u], preferred_element_type=f32)
        p = z * z
        p = p[:, :LANES] + p[:, LANES:]
        acc_ref[u] += p[:LANES] + p[LANES:]

    def both(taper, src, dst):
        def body(i, _):
            for j in range(UNROLL):
                second(UNROLL * i + j, src)
                first(UNROLL * i + j, taper, dst)
            return 0

        lax.fori_loop(0, UNITS // UNROLL, body, 0)

    def start(i, _):
        first(2 * i, 0, ga_ref)
        first(2 * i + 1, 0, ga_ref)
        return 0

    lax.fori_loop(0, chunks // 2, start, 0)

    def pair(i, _):
        both(2 * i + 1, ga_ref, gb_ref)
        both(jnp.minimum(2 * i + 2, tapers - 1), gb_ref, ga_ref)
        return 0

    lax.fori_loop(0, tapers // 2, pair, 0)

    for u in range(UNITS):
        t = (acc_ref[u].T * scale).astype(bf16)
        for d in range(groups):
            out_ref[d, u * rows_per : (u + 1) * rows_per, :] = t[d * rows_per : (d + 1) * rows_per]


def merge_kernel(rows, parts_ref, out_ref, sum_ref):
    groups = parts_ref.shape[0]
    for parity in range(2):
        total = parts_ref[parity].astype(f32)
        for g in range(parity + 2, groups, 2):
            total = total + parts_ref[g].astype(f32)
        sum_ref[:, parity * LANES : (parity + 1) * LANES] = total
    for i, r in enumerate(rows):
        out_ref[i : i + 1, :] = sum_ref[r : r + 1, :]


def merge_moments(mine, other, count):
    gap = other[0:1] - mine[0:1]
    row = lax.broadcasted_iota(jnp.int32, mine.shape, 0)
    both = mine + other
    return jnp.where(row == 0, both * 0.5, both + gap * gap * (count * 0.5))


def params(mib):
    return pltpu.CompilerParams(vmem_limit_bytes=mib * 2**20)


def local(signal, tapers, eigenvalues):
    row_count, chan_count = signal.shape
    taper_count, seg = tapers.shape
    stride = seg // 2
    tm = lax.axis_size("tm")
    chans = lax.axis_size("chan")
    blocks = row_count // LANES
    segments = row_count * tm // stride - 1
    half = chan_count // 2
    assert row_count == stride and half == LANES and seg == R * LANES

    sums = jnp.sum(signal.astype(f32), axis=1).reshape(blocks, LANES)
    if chans == 2:
        total = sums + lax.ppermute(sums, "chan", [(0, 1), (1, 0)])
    else:
        total = lax.psum(sums, "chan")
    common = total / (chan_count * chans)

    block_shape = jax.ShapeDtypeStruct((blocks, LANES, LANES), bf16)
    moments = jax.ShapeDtypeStruct((2, LANES), f32)
    keep, send, stats, send_stats = pl.pallas_call(
        prep_kernel,
        out_shape=(block_shape, block_shape, moments, moments),
        compiler_params=params(8),
        name="prep",
    )(signal, common)

    near_pairs = [(i, i ^ 1) for i in range(tm)]
    far_pairs = [(i, i + 1 if i % 2 else i - 1) for i in range(1, tm - 1)]
    other = lax.ppermute(send_stats, "tm", near_pairs)
    near = lax.ppermute(send, "tm", near_pairs)
    far = lax.ppermute(send, "tm", far_pairs)

    count = row_count
    stats = merge_moments(stats, other, count)
    count *= 2
    step = 2
    while tm // step > 4:
        other = lax.ppermute(stats, "tm", [(i, i ^ step) for i in range(tm)])
        stats = merge_moments(stats, other, count)
        count *= 2
        step *= 2
    parts = [stats] + [
        lax.ppermute(stats, "tm", [(i, i ^ (step * k)) for i in range(tm)])
        for k in range(1, tm // step)
    ]

    weights = eigenvalues / jnp.sum(eigenvalues)
    taps = (tapers.astype(f32) * jnp.sqrt(weights)[:, None]).reshape(taper_count, R, LANES)
    table = jnp.asarray(unit_tables(seg, tm))

    partial = pl.pallas_call(
        functools.partial(main_kernel, segments, count),
        out_shape=jax.ShapeDtypeStruct((tm, stride // tm, LANES), bf16),
        scratch_shapes=[
            pltpu.VMEM((2, taper_count, R, LANES), f32),
            pltpu.VMEM((3 * blocks, LANES, LANES), f32),
            pltpu.VMEM((UNITS, 2 * LANES, 2 * LANES), bf16),
            pltpu.VMEM((UNITS, 2 * LANES, 2 * LANES), bf16),
            pltpu.VMEM((UNITS, LANES, LANES), f32),
        ],
        compiler_params=params(24),
        name="spectra",
    )(keep, near, far, *parts, taps, table)

    got = lax.all_to_all(partial, "tm", 0, 0, tiled=True)
    rows = bin_rows(tm, seg)
    return pl.pallas_call(
        functools.partial(merge_kernel, rows),
        out_shape=jax.ShapeDtypeStruct((stride // tm, chan_count), f32),
        scratch_shapes=[pltpu.VMEM((stride // tm, chan_count), f32)],
        compiler_params=params(4),
        name="merge",
    )(got)


def solution(mesh):
    return jax.shard_map(
        local,
        mesh=mesh,
        in_specs=(P("tm", "chan"), P(), P()),
        out_specs=P("tm", "chan"),
        check_vma=False,
    )
```
